32 devices in a mesh: shard: 8 (over z, y), model: 4 (over x, core).
Axes of the slice: x: 2, y: 2, z: 4, core: 2. Of those that a mesh axis runs over, the one named last changes fastest.
Arguments:
- gradients: float32 [32, 128, 4096], P(None, 'shard', 'model'), may hold values from -6 to 6
- momentum: float32 [32, 128, 4096], P(None, 'shard', 'model'), may hold values from -6 to 6
- weights: float32 [32, 128, 4096], P(None, 'shard', 'model'), may hold values from -0.1875 to 0.1875
Outputs:
- new_weights: float32 [32, 128, 4096], P(None, 'shard', 'model')
- new_momentum: float32 [32, 128, 4096], P(None, 'shard', 'model')
The draws below stay inside these ranges and needn't reach their ends.
All inputs are finite; a program needn't handle non-finite values.
Results may differ from the reference program's by a relative error of at most 0.00015.
Values sent between devices are 32-bit elements; how exact they have to be, the bound alone decides.
No kernel may reach another device: no remote copies, remote signals or barrier semaphores. Data moves between devices by JAX's collectives and lax.ppermute only.
A program may use at most 128 MiB of HBM per device.

```python
import jax
import jax.numpy as jnp
from jax import lax

SIDE = 128
WIDE = 4096
MATS = 32
ITERS = 4


def level_of(stream_key, dims, cuts, low, top_value):
    def one(position, shards_of):
        steps = jax.random.uniform(jax.random.fold_in(jax.random.fold_in(stream_key, 6), position), (shards_of,), jnp.float32, low / len(cuts), top_value / len(cuts))
        return jnp.repeat(jnp.exp(steps), dims[position] // shards_of).reshape((-1,) + (1,) * (len(dims) - position - 1))

    level = one(*cuts[0])
    for cut in cuts[1:]:
        level = level * one(*cut)
    return level


def gaussian(rng, shape, width, reach, cuts=(), held_as=jnp.bfloat16):
    result = width * jax.random.normal(rng, shape, jnp.float32)
    if cuts:
        result = result * level_of(rng, shape, cuts, -0.22, 0.18)
    return jnp.clip(result, -reach, reach).astype(held_as)


def setup_inputs(seed: int = 0) -> dict:
    key_of = jax.random.split(jax.random.key(seed), 4)
    gradients = gaussian(key_of[0], (MATS, SIDE, WIDE), 1.0, 6.0, ((1, 8), (2, 4)), jnp.float32)
    momentum = gaussian(key_of[1], (MATS, SIDE, WIDE), 1.0, 6.0, ((1, 8), (2, 4)), jnp.float32)
    weights = gaussian(key_of[2], (MATS, SIDE, WIDE), 0.03, 0.1875, ((1, 8), (2, 4)), jnp.float32)
    return {"gradients": gradients, "momentum": momentum, "weights": weights}


hold_rate = 0.8
learn_rate = 1.0

def reference(gradients, momentum, weights):
    new_momentum = hold_rate * momentum + gradients

    def orthogonal_one(stack):
        iterate = stack[None]
        iterate = iterate * lax.rsqrt(lax.optimization_barrier(jnp.sum(iterate * iterate, axis=(1, 2), keepdims=True)) + 1e-06)
        for step in range(ITERS):
            gram = jnp.einsum('mik,mjk->mij', iterate, iterate, precision=lax.Precision.HIGHEST)
            mixed = -4.775 * gram + 2.0315 * jnp.einsum('mij,mjk->mik', gram, gram, precision=lax.Precision.HIGHEST)
            iterate = 3.4445 * iterate + jnp.einsum('mij,mjk->mik', mixed, iterate, precision=lax.Precision.HIGHEST)
        return iterate[0]
    iterate = lax.map(orthogonal_one, new_momentum)
    new_weights = weights - learn_rate * iterate
    return (new_weights, new_momentum)
```

```python
import jax
import jax.numpy as jnp
from jax import lax
from jax.sharding import PartitionSpec as P

ITERS = 4

hold_rate = 0.8
learn_rate = 1.0
HIGH = lax.Precision.HIGHEST


def mul(a, b):
    return jnp.einsum("mij,mjk->mik", a, b, precision=HIGH)


def direction(gram):
    eye = jnp.eye(gram.shape[-1], dtype=gram.dtype)
    squares = jnp.sum(gram * eye, axis=(1, 2), keepdims=True)
    scale = lax.rsqrt(squares + 1e-06)
    a = gram * scale * scale
    total = None
    for step in range(ITERS):
        q = 3.4445 * eye - 4.775 * a + 2.0315 * mul(a, a)
        total = q if total is None else mul(q, total)
        if step < ITERS - 1:
            a = mul(mul(q, a), q)
    return total * scale


def make(mesh):
    models = mesh.shape["model"]

    def on_device(gradients, momentum, weights):
        new_momentum = hold_rate * momentum + gradients
        whole = lax.all_to_all(new_momentum, "shard", split_axis=0, concat_axis=1, tiled=True)
        gram = jnp.einsum("mik,mjk->mij", whole, whole, precision=HIGH)
        mine = gram.shape[0] // models
        parts = lax.all_to_all(gram, "model", split_axis=0, concat_axis=0, tiled=True)
        gram = jnp.sum(parts.reshape(models, mine, *gram.shape[1:]), axis=0)
        turn = lax.all_gather(direction(gram), "model", axis=0, tiled=True)
        moved = mul(turn, whole)
        back = lax.all_to_all(moved, "shard", split_axis=1, concat_axis=0, tiled=True)
        new_weights = weights - learn_rate * back
        return (new_weights, new_momentum)

    return on_device


def solution(mesh):
    placed = P(None, "shard", "model")
    return jax.shard_map(
        make(mesh),
        mesh=mesh,
        in_specs=(placed, placed, placed),
        out_specs=(placed, placed),
        check_vma=False,
    )
```
